32 devices in a mesh: row: 4 (over y, x), col: 8 (over z, core).
Axes of the slice: x: 2, y: 2, z: 4, core: 2. Of those that a mesh axis runs over, the one named last changes fastest.
Arguments:
- panel: bfloat16 [131072, 256], P(('row', 'col')), may hold values from -6 to 6
- row_basis: bfloat16 [131072, 16], P('row'), may hold values from -1.5 to 1.5
- col_basis: bfloat16 [131072, 16], P(('row', 'col')), may hold values from -0.375 to 0.375
- near_blocks: bfloat16 [512, 9, 256, 256], P(('row', 'col')), may hold values from -0.125 to 0.125
- couplings: bfloat16 [4, 8, 512, 16, 16], P('row', 'col'), may hold values from -0.375 to 0.375
- blk_rows: int32 [4, 8, 512], P('row', 'col'), may hold values from 0 to 127
- blk_cols: int32 [4, 8, 512], P('row', 'col'), may hold values from 0 to 63
- blk_count: int32 [4, 8], P('row', 'col'), may hold values from 64 to 512, as said below
Outputs:
- product: bfloat16 [131072, 256], P(('row', 'col'))
The draws below stay inside these ranges and needn't reach their ends.
Inputs may be any that keep to these rules, and one draw needn't show every extreme that they name: `blk_count`: slots at or past a device's count hold in-range indices and are not part of the matrix; in every draw some device holds 512 live slots.
All inputs are finite; a program needn't handle non-finite values.
Results may differ from the reference program's by a relative error of at most 0.0052.
Values may be sent and summed in bfloat16 or wider, within the bound.
A program may use at most 192 MiB of HBM per device.

```python
import jax
import jax.numpy as jnp
from jax import lax

LEAF = 256
R = 16
NRHS = 256
HALF = 4
FAR_PER_CL = 32
CPD = 16
NEAR = 9
FAR_DEV = 512
NCL = 512
NPTS = 131072
N_ROW = 4
N_COL = 8


def draw_blk_count(key, part):
    first_key, second_key = jax.random.split(jax.random.fold_in(key, 17))
    raw_level = jax.random.randint(first_key, (N_ROW * N_COL,), 0, 64)
    lowest = FAR_DEV // 8
    counts = lowest + (FAR_DEV - lowest) * raw_level * raw_level // (63 * 63)
    fullest = jax.random.randint(second_key, (), 0, N_ROW * N_COL)
    counts = jnp.where(jnp.arange(N_ROW * N_COL) == fullest, FAR_DEV, counts)
    return counts.reshape(N_ROW, N_COL).astype(jnp.int32)


def set_ends(entries, key, low, largest):
    extent = entries.shape
    spot = [jax.random.randint(jax.random.fold_in(key, axis), (), 0, extent[axis]) for axis in range(len(extent))]
    entries = entries.at[tuple(spot)].set(low)
    longest = extent.index(max(extent))
    spot[longest] = (spot[longest] + 1) % extent[longest]
    return entries.at[tuple(spot)].set(largest)


def block_scale(rng, shape, shards, low, top_value):
    factor_of, own = 1.0, jax.random.fold_in(rng, 6)
    for axis_at, parts in shards:
        heights = jnp.exp(jax.random.uniform(jax.random.fold_in(own, axis_at), (parts,), jnp.float32, low / len(shards), top_value / len(shards)))
        factor_of = factor_of * jnp.repeat(heights, shape[axis_at] // parts).reshape([-1 if axis == axis_at else 1 for axis in range(len(shape))])
    return factor_of


def gaussian(key, shape, width, bound, pieces=(), held_as=jnp.bfloat16):
    values = jax.random.normal(key, shape, jnp.float32) * width
    if len(pieces) > 0:
        values = block_scale(key, shape, pieces, -0.22, 0.18) * values
    return jnp.clip(values, min=-bound, max=bound).astype(held_as)


def setup_inputs(seed: int = 0) -> dict:
    seeds = jax.random.split(jax.random.key(seed), 9)
    return {
        "panel": gaussian(seeds[0], (NPTS, NRHS), 1.0, 6.0, ((0, 32),)),
        "row_basis": gaussian(seeds[1], (NPTS, R), R ** -0.5, 1.5, ((0, 4),)),
        "col_basis": gaussian(seeds[2], (NPTS, R), LEAF ** -0.5, 0.375, ((0, 32),)),
        "near_blocks": gaussian(seeds[3], (NCL, NEAR, LEAF, LEAF), (NEAR * LEAF) ** -0.5, 0.125, ((0, 32),)),
        "couplings": gaussian(seeds[4], (N_ROW, N_COL, FAR_DEV, R, R), (R * FAR_PER_CL // 2) ** -0.5, 0.375, ((0, 4), (1, 8))),
        "blk_rows": set_ends(jax.random.randint(seeds[5], (N_ROW, N_COL, FAR_DEV), 0, N_COL * CPD), jax.random.fold_in(seeds[5], 1), 0, (N_COL * CPD) - 1).astype(jnp.int32),
        "blk_cols": set_ends(jax.random.randint(seeds[6], (N_ROW, N_COL, FAR_DEV), 0, N_ROW * CPD), jax.random.fold_in(seeds[6], 1), 0, (N_ROW * CPD) - 1).astype(jnp.int32),
        "blk_count": draw_blk_count(jax.random.fold_in(seeds[8], 71), 0),
    }


def reference(panel, row_basis, col_basis, near_blocks, couplings, blk_rows, blk_cols, blk_count):
    cluster_total = NPTS // LEAF
    highest = lax.Precision.HIGHEST
    clusters = panel.reshape(cluster_total, LEAF, NRHS).astype(jnp.float32)
    coeffs = jnp.einsum('kpr,kpn->krn', col_basis.reshape(cluster_total, LEAF, R).astype(jnp.float32), clusters, precision=highest).astype(jnp.bfloat16)
    owner_row = jnp.arange(N_ROW, dtype=jnp.int32)[:, None, None]
    owner_col = jnp.arange(N_COL, dtype=jnp.int32)[None, :, None]
    global_row = owner_row * (N_COL * CPD) + blk_rows
    global_col = ((blk_cols // CPD) * N_COL + owner_col) * CPD + blk_cols % CPD
    is_live = jnp.arange(FAR_DEV, dtype=jnp.int32)[None, None, :] < blk_count[:, :, None]
    slot_total = N_ROW * N_COL * FAR_DEV
    picked = coeffs[global_col.reshape(slot_total)].astype(jnp.float32)
    block_terms = jnp.einsum('bij,bjn->bin', couplings.reshape(slot_total, R, R).astype(jnp.float32), picked, precision=highest)
    block_terms = jnp.where(is_live.reshape(slot_total)[:, None, None], block_terms, jnp.float32(0.0))
    coupled = jax.ops.segment_sum(block_terms, global_row.reshape(slot_total), num_segments=cluster_total)
    far_field = jnp.einsum('kpr,krn->kpn', row_basis.reshape(cluster_total, LEAF, R).astype(jnp.float32), coupled, precision=highest)
    padded = jnp.pad(clusters, ((HALF, HALF), (0, 0), (0, 0)))
    near_field = jnp.zeros((cluster_total, LEAF, NRHS), jnp.float32)
    for offset in range(NEAR):
        near_field = near_field + jnp.einsum('kpq,kqn->kpn', near_blocks[:, offset].astype(jnp.float32), padded[offset:offset + cluster_total], precision=highest)
    return (near_field + far_field).reshape(NPTS, NRHS).astype(jnp.bfloat16)
```

```python
import functools

import jax
import jax.numpy as jnp
from jax import lax
from jax.experimental import pallas as pl
from jax.experimental.pallas import tpu as pltpu
from jax.sharding import PartitionSpec as P

MESH = pl.DeviceIdType.MESH
BF16 = jnp.bfloat16
F32 = jnp.float32


def dot(left, right, contract=((1,), (0,))):
    return lax.dot_general(left, right, (contract, ((), ())), preferred_element_type=F32)


def kernel(
    nr, nc,
    panel, row_t, col_t, near, coup, rows, cols, count,
    near_sum, wide, total,
    blocks, win, dense, coeffs, spread, pick,
    coup_v, row_v, col_v, rows_v, cols_v, count_v,
    give, own, pair_in, chip_sum, far_in, summed,
    near_sem, in_sem, gs, gr, hs, hr, xs, xr, us, ur, ready,
):
    clusters, near_count, leaf, _ = blocks.shape
    half = near_count // 2
    rank = col_v.shape[0]
    slots = rows_v.shape[1]
    nz = nc // 2
    group_rows = nc * clusters
    group_cols = nr * clusters
    block = rank * clusters
    r = lax.axis_index("row")
    c = lax.axis_index("col")
    line = r * nc + c
    z = c // 2
    e = c % 2
    has_next = line < nr * nc - 1
    has_prev = line > 0
    next_id = (jnp.minimum(line + 1, nr * nc - 1) // nc, (c + 1) % nc)
    prev_id = (jnp.maximum(line - 1, 0) // nc, (c + nc - 1) % nc)
    pair_id = (r, z * 2 + 1 - e)
    lower, upper = e == 0, e == 1
    first, last = z == 0, z == nz - 1
    PAIR, SIDE, LINE = nr - 1, nr, nr + 1
    barrier = pltpu.get_barrier_semaphore()

    def signal(sem, to):
        pl.semaphore_signal(sem, inc=1, device_id=to, device_id_type=MESH)

    def row_id(d):
        return ((r + d) % nr, c)

    with jax.named_scope("greet"):
        for d in range(1, nr):
            @pl.when(r + d < nr)
            def _(d=d):
                signal(barrier, row_id(d))

        @pl.when(lower)
        def _():
            signal(barrier, pair_id)

        for t in range(1, nz):
            @pl.when(t > z)
            def _(t=t):
                signal(barrier, (r, t * 2 + e))

        @pl.when(upper & ~last)
        def _():
            signal(barrier, next_id)

        @pl.when(lower & first & has_prev)
        def _():
            signal(barrier, prev_id)

    own_win = win.at[pl.ds(half, clusters)]
    loads = [
        pltpu.make_async_copy(panel, own_win, in_sem.at[0]),
        pltpu.make_async_copy(col_t, col_v, in_sem.at[1]),
        pltpu.make_async_copy(coup, coup_v, in_sem.at[2]),
        pltpu.make_async_copy(rows, rows_v, in_sem.at[3]),
        pltpu.make_async_copy(cols, cols_v, in_sem.at[4]),
        pltpu.make_async_copy(count, count_v, in_sem.at[5]),
        pltpu.make_async_copy(
            row_t.at[:, pl.ds(pl.multiple_of(c * clusters * leaf, 128), clusters * leaf)],
            row_v, in_sem.at[6],
        ),
    ]
    with jax.named_scope("loads"):
        for load in loads:
            load.start()

    def near_load(k):
        return pltpu.make_async_copy(near.at[k], blocks.at[k], near_sem.at[k])

    def start_near(step, carry):
        near_load((step + half) % clusters).start()
        return carry

    tail = pltpu.make_async_remote_copy(
        panel.at[pl.ds(clusters - half, half)], win.at[pl.ds(0, half)], hs.at[0], hr.at[0],
        device_id=next_id, device_id_type=MESH,
    )
    head = pltpu.make_async_remote_copy(
        panel.at[pl.ds(0, half)], win.at[pl.ds(half + clusters, half)], hs.at[1], hr.at[1],
        device_id=prev_id, device_id_type=MESH,
    )

    with jax.named_scope("barrier"):
        one = jnp.int32(1)
        zero = jnp.int32(0)
        earlier = (
            r + z + jnp.where(upper, one, zero)
            + jnp.where(lower & ~first, one, zero) + jnp.where(upper & last & has_next, one, zero)
        )

        @pl.when(earlier > 0)
        def _():
            pl.semaphore_wait(barrier, earlier)

        for d in range(1, nr):
            @pl.when(r + d >= nr)
            def _(d=d):
                signal(ready.at[nr - 1 - d], row_id(d))

        @pl.when(upper)
        def _():
            signal(ready.at[PAIR], pair_id)

        for t in range(nz - 1):
            @pl.when(t < z)
            def _(t=t):
                signal(ready.at[LINE + z], (r, t * 2 + e))

        @pl.when(lower & ~first)
        def _():
            signal(ready.at[SIDE], prev_id)
            head.start()

        @pl.when(upper & last & has_next)
        def _():
            signal(ready.at[SIDE], next_id)
            tail.start()

        @pl.when(upper)
        def _():
            head.start()

        lax.fori_loop(0, clusters, start_near, 0)

    def gather_copy(d):
        return pltpu.make_async_remote_copy(
            coeffs.at[r], coeffs.at[r], gs.at[d - 1], gr.at[d - 1],
            device_id=row_id(d), device_id_type=MESH,
        )

    with jax.named_scope("panel_wait"):
        for load in loads[:2]:
            load.wait()

    pieces = 2
    per = clusters // pieces
    for piece in range(pieces):
        with jax.named_scope("coeffs"):
            for k in range(piece * per, (piece + 1) * per):
                coeffs[r, k * rank : (k + 1) * rank, :] = dot(
                    col_v[:, k * leaf : (k + 1) * leaf], win[half + k]
                ).astype(BF16)
        if piece == 0:
            with jax.named_scope("side"):
                @pl.when(upper & ~last)
                def _():
                    pl.semaphore_wait(ready.at[SIDE], 1)
                    tail.start()

                @pl.when(lower)
                def _():
                    pl.semaphore_wait(ready.at[PAIR], 1)
                    tail.start()

    with jax.named_scope("gather"):
        for d in range(nr - 1, 0, -1):
            @pl.when(r + d < nr)
            def _(d=d):
                pl.semaphore_wait(ready.at[d - 1], 1)

            gather_copy(d).start()

    with jax.named_scope("spread"):
        for load in loads[2:6]:
            load.wait()
        col_ids = cols_v[...]
        live = lax.broadcasted_iota(jnp.int32, (1, slots), 1) < count_v[0, 0]
        picked = jnp.where(live, col_ids // clusters * group_rows + rows_v[...], -1)
        col_ids = col_ids % clusters

        def pick_step(m, carry):
            at = lax.broadcasted_iota(jnp.int32, (clusters, slots), 0) + m * clusters
            hit = jnp.where(at == picked, 1.0, 0.0).astype(BF16)
            pick[pl.ds(pl.multiple_of(m * clusters, clusters), clusters), :] = hit
            return carry

        lax.fori_loop(0, nr * nc, pick_step, 0, unroll=8)
        for j in range(clusters):
            spread[j] = jnp.where(jnp.broadcast_to(col_ids, (rank, slots)) == j, 1.0, 0.0).astype(BF16)

    def dense_step(a, carry):
        placed = (spread[...] * coup_v[a][None]).reshape(block, slots)
        part = dot(pick[...], placed, ((1,), (1,))).astype(BF16)
        at = pl.ds(pl.multiple_of(a * clusters, clusters), clusters)
        for s in range(nr):
            dense[:, at, s * block : (s + 1) * block] = part[s * group_rows : (s + 1) * group_rows].reshape(
                nc, clusters, block
            )
        return carry

    with jax.named_scope("dense0"):
        lax.fori_loop(0, rank // 2, dense_step, 0, unroll=2)

    with jax.named_scope("wrap"):
        @pl.when(lower & first & has_prev)
        def _():
            pl.semaphore_wait(ready.at[SIDE], 1)
            head.start()

    with jax.named_scope("dense1"):
        lax.fori_loop(rank // 2, rank, dense_step, 0, unroll=2)

    def near_step(k, carry):
        near_load(k).wait()
        left = jnp.concatenate([blocks[k, o] for o in range(near_count)], axis=1)
        right = win[pl.ds(k, near_count)].reshape(near_count * leaf, win.shape[2])
        near_sum[k] = dot(left, right)
        return carry

    def wide_step(k, carry):
        at = lax.broadcasted_iota(jnp.int32, (rank, block), 0)
        to = lax.broadcasted_iota(jnp.int32, (rank, block), 1)
        place = jnp.where(to == at * clusters + k, 1.0, 0.0).astype(BF16)
        mine = row_v[:, pl.ds(pl.multiple_of(k * leaf, leaf), leaf)]
        wide[k] = dot(mine, place, ((0,), (0,))).astype(BF16)
        return carry

    with jax.named_scope("wide"):
        loads[6].wait()
        lax.fori_loop(0, clusters, wide_step, 0, unroll=4)
    early = half + (clusters - 2 * half) // 4
    with jax.named_scope("near_early"):
        lax.fori_loop(half, early, near_step, 0)

    with jax.named_scope("gather_wait"):
        for d in range(1, nr):
            gather_copy(d).wait_recv()

    def target(j):
        return jnp.where(z < nz // 2, nz - 1 - j, j)

    def partial_for(column):
        return dot(dense[column], coeffs[...].reshape(group_cols * rank, coeffs.shape[2]))

    def pair_copy(t):
        return pltpu.make_async_remote_copy(
            give.at[t], pair_in.at[t], xs.at[t], xr.at[t], device_id=pair_id, device_id_type=MESH
        )

    def far_copy(t):
        return pltpu.make_async_remote_copy(
            chip_sum.at[t], far_in.at[z], us.at[t], ur.at[z],
            device_id=(r, t * 2 + e), device_id_type=MESH,
        )

    def give_step(j, carry):
        t = target(j)
        give[t] = partial_for(t * 2 + 1 - e).astype(BF16)
        pair_copy(t).start()
        return carry

    with jax.named_scope("give"):
        lax.fori_loop(0, nz, give_step, 0)

    def send_step(j, carry):
        t = target(j)
        own[...] = partial_for(t * 2 + e)
        pair_copy(t).wait_recv()
        value = own[...] + pair_in[t].astype(F32)

        @pl.when(t != z)
        def _():
            chip_sum[t] = value.astype(BF16)

            @pl.when(t > z)
            def _():
                pl.semaphore_wait(ready.at[LINE + t], 1)

            far_copy(t).start()

        @pl.when(t == z)
        def _():
            summed[...] = value

        return carry

    with jax.named_scope("send"):
        lax.fori_loop(0, nz, send_step, 0)

    with jax.named_scope("near0"):
        lax.fori_loop(early, clusters - half, near_step, 0)

    def take_front():
        @pl.when(has_prev)
        def _():
            tail.wait_recv()

        @pl.when(~has_prev)
        def _():
            win[pl.ds(0, half)] = jnp.zeros((half, leaf, win.shape[2]), BF16)

    def take_back():
        @pl.when(has_next)
        def _():
            head.wait_recv()

        @pl.when(~has_next)
        def _():
            win[pl.ds(half + clusters, half)] = jnp.zeros((half, leaf, win.shape[2]), BF16)

    def edge_step(base):
        def step(k, carry):
            return near_step(base + k, carry)
        return step

    with jax.named_scope("near1"):
        pl.when(lower)(take_back)
        pl.when(upper)(take_front)
        lax.fori_loop(0, half, edge_step(jnp.where(lower, clusters - half, 0)), 0)
    with jax.named_scope("halo_wait"):
        pl.when(upper)(take_back)
        pl.when(lower)(take_front)
    with jax.named_scope("near2"):
        lax.fori_loop(0, half, edge_step(jnp.where(lower, 0, clusters - half)), 0)

    def take_step(j, carry):
        s = jnp.where(z < nz // 2, j, nz - 1 - j)

        @pl.when(s != z)
        def _():
            pltpu.make_async_remote_copy(
                chip_sum.at[s], far_in.at[s], us.at[s], ur.at[s],
                device_id=(r, s * 2 + e), device_id_type=MESH,
            ).wait_recv()
            summed[...] += far_in[s].astype(F32)

        return carry

    with jax.named_scope("take"):
        lax.fori_loop(0, nz, take_step, 0)
    with jax.named_scope("total"):
        total[...] = summed[...].astype(BF16)

    with jax.named_scope("drain"):
        for d in range(1, nr):
            gather_copy(d).wait_send()

        @pl.when(has_next)
        def _():
            tail.wait_send()

        @pl.when(has_prev)
        def _():
            head.wait_send()

        def sent_step(t, carry):
            pair_copy(t).wait_send()

            @pl.when(t != z)
            def _():
                far_copy(t).wait_send()

            return carry

        lax.fori_loop(0, nz, sent_step, 0)


def finish(near_sum, wide, total, out, held, sem):
    clusters, leaf, _ = held.shape

    def copy(k):
        return pltpu.make_async_copy(held.at[k], out.at[pl.ds(pl.multiple_of(k * leaf, leaf), leaf)], sem.at[k])

    for k in range(clusters):
        held[k] = (near_sum[k] + dot(wide[k], total[...])).astype(BF16)
        copy(k).start()
    for k in range(clusters):
        copy(k).wait()


def on_device(nr, nc, panel, row_basis, col_basis, near_blocks, couplings, blk_rows, blk_cols, blk_count):
    own_rows, width = panel.shape
    clusters, near_count, leaf, _ = near_blocks.shape
    half = near_count // 2
    rank = col_basis.shape[1]
    slots = couplings.shape[2]
    nz = nc // 2
    block = rank * clusters
    group_rows, group_cols = nc * clusters, nr * clusters
    dma = pltpu.SemaphoreType.DMA
    vmem = pl.BlockSpec(memory_space=pltpu.VMEM)
    near_sum, wide, total = pl.pallas_call(
        functools.partial(kernel, nr, nc),
        out_shape=(
            pltpu.VMEM((clusters, leaf, width), F32),
            pltpu.VMEM((clusters, leaf, block), BF16),
            pltpu.VMEM((block, width), BF16),
        ),
        in_specs=[pl.BlockSpec(memory_space=pl.ANY)] * 7 + [pl.BlockSpec(memory_space=pltpu.HBM)],
        out_specs=[vmem] * 3,
        scratch_shapes=[
            pltpu.VMEM(near_blocks.shape, BF16),
            pltpu.VMEM((clusters + 2 * half, leaf, width), BF16),
            pltpu.VMEM((nc, block, group_cols * rank), BF16),
            pltpu.VMEM((nr, block, width), BF16),
            pltpu.VMEM((clusters, rank, slots), BF16),
            pltpu.VMEM((nr * group_rows, slots), BF16),
            pltpu.VMEM((rank, rank, slots), BF16),
            pltpu.VMEM((rank, own_rows), BF16),
            pltpu.VMEM((rank, own_rows), BF16),
            pltpu.VMEM((1, slots), jnp.int32),
            pltpu.VMEM((1, slots), jnp.int32),
            pltpu.SMEM((1, 1), jnp.int32),
            pltpu.VMEM((nz, block, width), BF16),
            pltpu.VMEM((block, width), F32),
            pltpu.VMEM((nz, block, width), BF16),
            pltpu.VMEM((nz, block, width), BF16),
            pltpu.VMEM((nz, block, width), BF16),
            pltpu.VMEM((block, width), F32),
            dma((clusters,)),
            dma((7,)),
            dma((max(nr - 1, 1),)),
            dma((max(nr - 1, 1),)),
            dma((2,)),
            dma((2,)),
            dma((nz,)),
            dma((nz,)),
            dma((nz,)),
            dma((nz,)),
            pltpu.SemaphoreType.REGULAR((nr + 1 + nz,)),
        ],
        compiler_params=pltpu.CompilerParams(
            collective_id=0, has_side_effects=True, vmem_limit_bytes=VMEM_BYTES
        ),
    )(
        panel.reshape(clusters, leaf, width),
        row_basis.T,
        col_basis.T,
        near_blocks,
        couplings.reshape(slots, rank, rank).transpose(1, 2, 0),
        blk_rows.reshape(1, slots),
        blk_cols.reshape(1, slots),
        blk_count,
    )
    return pl.pallas_call(
        finish,
        out_shape=jax.ShapeDtypeStruct((own_rows, width), BF16),
        in_specs=[vmem] * 3,
        out_specs=pl.BlockSpec(memory_space=pl.ANY),
        scratch_shapes=[pltpu.VMEM((clusters, leaf, width), BF16), dma((clusters,))],
        compiler_params=pltpu.CompilerParams(vmem_limit_bytes=16 << 20),
    )(near_sum, wide, total)


VMEM_BYTES = 56 << 20


def solution(mesh):
    placed = (
        P(("row", "col"), None),
        P("row", None),
        P(("row", "col"), None),
        P(("row", "col"), None, None, None),
        P("row", "col", None, None, None),
        P("row", "col", None),
        P("row", "col", None),
        P("row", "col"),
    )
    return jax.shard_map(
        functools.partial(on_device, mesh.shape["row"], mesh.shape["col"]),
        mesh=mesh, in_specs=placed, out_specs=P(("row", "col"), None), check_vma=False,
    )
```

```python
import functools

import jax
import jax.numpy as jnp
from jax import lax
from jax.experimental import pallas as pl
from jax.experimental.pallas import tpu as pltpu
from jax.sharding import PartitionSpec as P

MESH = pl.DeviceIdType.MESH
BF16 = jnp.bfloat16
F32 = jnp.float32


def dot(left, right, contract=((1,), (0,))):
    return lax.dot_general(left, right, (contract, ((), ())), preferred_element_type=F32)


def kernel(
    nr, nc,
    panel, row_t, col_t, near, coup, rows, cols, count,
    near_sum, wide, total,
    blocks, win, dense, coeffs, spread, pick,
    coup_v, row_v, col_v, rows_v, cols_v, count_v,
    give, own, pair_in, chip_sum, far_in, summed, kept, relay_in,
    near_sem, in_sem, gs, gr, hs, hr, xs, xr, us, ur, rs, rr, ready,
):
    clusters, near_count, leaf, _ = blocks.shape
    half = near_count // 2
    rank = col_v.shape[0]
    slots = rows_v.shape[1]
    nz = nc // 2
    group_rows = nc * clusters
    group_cols = nr * clusters
    block = rank * clusters
    r = lax.axis_index("row")
    c = lax.axis_index("col")
    line = r * nc + c
    z = c // 2
    e = c % 2
    has_next = line < nr * nc - 1
    has_prev = line > 0
    next_id = (jnp.minimum(line + 1, nr * nc - 1) // nc, (c + 1) % nc)
    prev_id = (jnp.maximum(line - 1, 0) // nc, (c + nc - 1) % nc)
    pair_id = (r, z * 2 + 1 - e)
    lower, upper = e == 0, e == 1
    first, last = z == 0, z == nz - 1
    PAIR, SIDE, LINE = nr - 1, nr, nr + 1
    barrier = pltpu.get_barrier_semaphore()

    def signal(sem, to):
        pl.semaphore_signal(sem, inc=1, device_id=to, device_id_type=MESH)

    def row_id(d):
        return ((r + d) % nr, c)

    with jax.named_scope("greet"):
        for d in range(1, nr):
            @pl.when(r + d < nr)
            def _(d=d):
                signal(barrier, row_id(d))

        @pl.when(lower)
        def _():
            signal(barrier, pair_id)

        for t in range(1, nz):
            @pl.when(t > z)
            def _(t=t):
                signal(barrier, (r, t * 2 + e))

        @pl.when(upper & ~last)
        def _():
            signal(barrier, next_id)

        @pl.when(lower & first & has_prev)
        def _():
            signal(barrier, prev_id)

    own_win = win.at[pl.ds(half, clusters)]
    loads = [
        pltpu.make_async_copy(col_t, col_v, in_sem.at[1]),
        pltpu.make_async_copy(coup, coup_v, in_sem.at[2]),
        pltpu.make_async_copy(rows, rows_v, in_sem.at[3]),
        pltpu.make_async_copy(cols, cols_v, in_sem.at[4]),
        pltpu.make_async_copy(count, count_v, in_sem.at[5]),
        pltpu.make_async_copy(
            row_t.at[:, pl.ds(pl.multiple_of(c * clusters * leaf, 128), clusters * leaf)],
            row_v, in_sem.at[6],
        ),
    ]
    pieces = 2
    per = clusters // pieces
    panel_loads = [
        pltpu.make_async_copy(
            panel.at[pl.ds(p * per, per)], own_win.at[pl.ds(p * per, per)], in_sem.at[(0, 7)[p]]
        )
        for p in range(pieces)
    ]
    with jax.named_scope("loads"):
        loads[0].start()
        for load in panel_loads + loads[1:]:
            load.start()

    def near_load(k):
        return pltpu.make_async_copy(near.at[k], blocks.at[k], near_sem.at[k])

    def start_near(step, carry):
        near_load((step + half) % clusters).start()
        return carry

    tail = pltpu.make_async_remote_copy(
        panel.at[pl.ds(clusters - half, half)], win.at[pl.ds(0, half)], hs.at[0], hr.at[0],
        device_id=next_id, device_id_type=MESH,
    )
    head = pltpu.make_async_remote_copy(
        panel.at[pl.ds(0, half)], win.at[pl.ds(half + clusters, half)], hs.at[1], hr.at[1],
        device_id=prev_id, device_id_type=MESH,
    )

    with jax.named_scope("barrier"):
        one = jnp.int32(1)
        zero = jnp.int32(0)
        earlier = (
            r + z + jnp.where(upper, one, zero)
            + jnp.where(lower & ~first, one, zero) + jnp.where(upper & last & has_next, one, zero)
        )

        @pl.when(earlier > 0)
        def _():
            pl.semaphore_wait(barrier, earlier)

        for d in range(1, nr):
            @pl.when(r + d >= nr)
            def _(d=d):
                signal(ready.at[nr - 1 - d], row_id(d))

        @pl.when(upper)
        def _():
            signal(ready.at[PAIR], pair_id)

        for t in range(nz - 1):
            @pl.when(t < z)
            def _(t=t):
                signal(ready.at[LINE + z], (r, t * 2 + e))

        @pl.when(lower & ~first)
        def _():
            signal(ready.at[SIDE], prev_id)
            head.start()

        @pl.when(upper & last & has_next)
        def _():
            signal(ready.at[SIDE], next_id)

        @pl.when(upper)
        def _():
            head.start()

        lax.fori_loop(0, clusters, start_near, 0)

    def gather_copy(d, at=None):
        part = coeffs.at[r] if at is None else coeffs.at[r, pl.ds(at * per * rank, per * rank)]
        return pltpu.make_async_remote_copy(
            part, part, gs.at[d - 1], gr.at[d - 1],
            device_id=row_id(d), device_id_type=MESH,
        )

    with jax.named_scope("panel_wait"):
        loads[0].wait()

    for piece in range(pieces):
        with jax.named_scope("coeffs"):
            panel_loads[piece].wait()
            for k in range(piece * per, (piece + 1) * per):
                coeffs[r, k * rank : (k + 1) * rank, :] = dot(
                    col_v[:, k * leaf : (k + 1) * leaf], win[half + k]
                ).astype(BF16)
        for d in range(1, nr):
            @pl.when(r + d >= nr)
            def _(d=d, piece=piece):
                gather_copy(d, piece).start()

        if piece == 0:
            with jax.named_scope("side"):
                @pl.when(upper & ~last)
                def _():
                    pl.semaphore_wait(ready.at[SIDE], 1)
                    tail.start()

                @pl.when(lower)
                def _():
                    pl.semaphore_wait(ready.at[PAIR], 1)
                    tail.start()

    with jax.named_scope("gather"):
        for d in range(1, nr):
            @pl.when(r + d < nr)
            def _(d=d):
                pl.semaphore_wait(ready.at[d - 1], 1)
                for piece in range(pieces):
                    gather_copy(d, piece).start()

    with jax.named_scope("spread"):
        for load in loads[1:5]:
            load.wait()
        col_ids = cols_v[...]
        live = lax.broadcasted_iota(jnp.int32, (1, slots), 1) < count_v[0, 0]
        picked = jnp.where(live, col_ids // clusters * group_rows + rows_v[...], -1)
        col_ids = col_ids % clusters

        def pick_step(m, carry):
            at = lax.broadcasted_iota(jnp.int32, (clusters, slots), 0) + m * clusters
            hit = jnp.where(at == picked, 1.0, 0.0).astype(BF16)
            pick[pl.ds(pl.multiple_of(m * clusters, clusters), clusters), :] = hit
            return carry

        lax.fori_loop(0, nr * nc, pick_step, 0, unroll=8)
        for j in range(clusters):
            spread[j] = jnp.where(jnp.broadcast_to(col_ids, (rank, slots)) == j, 1.0, 0.0).astype(BF16)

    @pl.when(upper & last & has_next)
    def _():
        tail.start()

    def dense_step(a, carry):
        placed = (spread[...] * coup_v[a][None]).reshape(block, slots)
        part = dot(pick[...], placed, ((1,), (1,))).astype(BF16)
        at = pl.ds(pl.multiple_of(a * clusters, clusters), clusters)
        for s in range(nr):
            dense[:, at, s * block : (s + 1) * block] = part[s * group_rows : (s + 1) * group_rows].reshape(
                nc, clusters, block
            )
        return carry

    with jax.named_scope("dense0"):
        lax.fori_loop(0, rank // 2, dense_step, 0, unroll=2)

    with jax.named_scope("dense1"):
        lax.fori_loop(rank // 2, rank, dense_step, 0, unroll=2)

    def near_step(k, carry):
        near_load(k).wait()
        left = jnp.concatenate([blocks[k, o] for o in range(near_count)], axis=1)
        right = win[pl.ds(k, near_count)].reshape(near_count * leaf, win.shape[2])
        near_sum[k] = dot(left, right)
        return carry

    def wide_step(k, carry):
        at = lax.broadcasted_iota(jnp.int32, (rank, block), 0)
        to = lax.broadcasted_iota(jnp.int32, (rank, block), 1)
        place = jnp.where(to == at * clusters + k, 1.0, 0.0).astype(BF16)
        mine = row_v[:, pl.ds(pl.multiple_of(k * leaf, leaf), leaf)]
        wide[k] = dot(mine, place, ((0,), (0,))).astype(BF16)
        return carry

    with jax.named_scope("wrap"):
        @pl.when(lower & first & has_prev)
        def _():
            pl.semaphore_wait(ready.at[SIDE], 1)
            head.start()

    with jax.named_scope("wide"):
        loads[5].wait()
        lax.fori_loop(0, clusters, wide_step, 0, unroll=4)
    early = half + (clusters - 2 * half) // 4
    with jax.named_scope("near_early"):
        lax.fori_loop(half, early, near_step, 0)

    with jax.named_scope("gather_wait"):
        for d in range(1, nr):
            gather_copy(d).wait_recv()

    relayed = nz > 2
    up_to, down_to = 2, nz - 3

    def target(j):
        far_first = jnp.where(z < nz // 2, nz - 1 - j, j)
        if not relayed:
            return far_first
        skip = nz - j
        apart = jnp.where(j == 0, up_to, jnp.where(skip > up_to, skip, skip - 1))
        near_first = jnp.where(j == 0, 0, nz - j)
        inner = jnp.where(z < nz // 2, near_first, far_first)
        return jnp.where(first, apart, jnp.where(last, nz - 1 - apart, inner))

    def hands_up(t):
        return first & (t == up_to) if relayed else False

    def hands_down(t):
        return last & (t == down_to) if relayed else False

    def partial_for(column):
        return dot(dense[column], coeffs[...].reshape(group_cols * rank, coeffs.shape[2]))

    def pair_copy(t):
        return pltpu.make_async_remote_copy(
            give.at[t], pair_in.at[t], xs.at[t], xr.at[t], device_id=pair_id, device_id_type=MESH
        )

    def far_copy(t):
        return pltpu.make_async_remote_copy(
            chip_sum.at[t], far_in.at[z], us.at[t], ur.at[z],
            device_id=(r, t * 2 + e), device_id_type=MESH,
        )

    def give_step(j, carry):
        t = target(j)
        give[t] = partial_for(t * 2 + 1 - e).astype(BF16)
        pair_copy(t).start()
        return carry

    with jax.named_scope("give"):
        for t in range(1, nz):
            @pl.when(t > z)
            def _(t=t):
                pl.semaphore_wait(ready.at[LINE + t], 1)

        lax.fori_loop(0, nz, give_step, 0)

    def up_copy():
        return pltpu.make_async_remote_copy(
            chip_sum.at[up_to], relay_in.at[0], rs.at[0], rr.at[0],
            device_id=(r, 2 + e), device_id_type=MESH,
        )

    def down_copy():
        return pltpu.make_async_remote_copy(
            chip_sum.at[down_to], relay_in.at[1], rs.at[1], rr.at[1],
            device_id=(r, (nz - 2) * 2 + e), device_id_type=MESH,
        )

    def send_step(j, carry):
        t = target(j)
        own[...] = partial_for(t * 2 + e)
        pair_copy(t).wait_recv()
        value = own[...] + pair_in[t].astype(F32)
        direct = t != z
        if relayed:
            keeps_up = (z == 1) & (t == up_to)
            keeps_down = (z == nz - 2) & (t == down_to)
            direct &= ~(keeps_up | keeps_down)

            @pl.when(keeps_up)
            def _():
                kept[0] = value

            @pl.when(keeps_down)
            def _():
                kept[1] = value

        @pl.when(t == z)
        def _():
            summed[...] = value

        @pl.when(direct)
        def _():
            chip_sum[t] = value.astype(BF16)

            if relayed:
                @pl.when(hands_up(t))
                def _():
                    up_copy().start()

                @pl.when(hands_down(t))
                def _():
                    down_copy().start()

                @pl.when(~(hands_up(t) | hands_down(t)))
                def _():
                    far_copy(t).start()
            else:
                far_copy(t).start()

        return carry

    with jax.named_scope("send"):
        lax.fori_loop(0, nz, send_step, 0)

    with jax.named_scope("near0"):
        lax.fori_loop(early, clusters - half, near_step, 0)

    def relay():
        @pl.when(z == 1)
        def _():
            up_copy().wait_recv()
            chip_sum[up_to] = (kept[0] + relay_in[0].astype(F32)).astype(BF16)
            far_copy(up_to).start()

        @pl.when(z == nz - 2)
        def _():
            down_copy().wait_recv()
            chip_sum[down_to] = (kept[1] + relay_in[1].astype(F32)).astype(BF16)
            far_copy(down_to).start()

    def take_front():
        @pl.when(has_prev)
        def _():
            tail.wait_recv()

        @pl.when(~has_prev)
        def _():
            win[pl.ds(0, half)] = jnp.zeros((half, leaf, win.shape[2]), BF16)

    def take_back():
        @pl.when(has_next)
        def _():
            head.wait_recv()

        @pl.when(~has_next)
        def _():
            win[pl.ds(half + clusters, half)] = jnp.zeros((half, leaf, win.shape[2]), BF16)

    def edge_step(base):
        def step(k, carry):
            return near_step(base + k, carry)
        return step

    with jax.named_scope("near1"):
        pl.when(lower)(take_back)
        pl.when(upper)(take_front)
        lax.fori_loop(0, half, edge_step(jnp.where(lower, clusters - half, 0)), 0)
    with jax.named_scope("halo_wait"):
        pl.when(upper)(take_back)
        pl.when(lower)(take_front)
    with jax.named_scope("near2"):
        lax.fori_loop(0, half, edge_step(jnp.where(lower, 0, clusters - half)), 0)

    if relayed:
        with jax.named_scope("relay"):
            relay()

    def take_step(j, carry):
        s = jnp.where(z < nz // 2, j, nz - 1 - j)
        direct = s != z
        if relayed:
            direct &= ~(((z == up_to) & (s == 0)) | ((z == down_to) & (s == nz - 1)))

        @pl.when(direct)
        def _():
            pltpu.make_async_remote_copy(
                chip_sum.at[s], far_in.at[s], us.at[s], ur.at[s],
                device_id=(r, s * 2 + e), device_id_type=MESH,
            ).wait_recv()
            summed[...] += far_in[s].astype(F32)

        return carry

    with jax.named_scope("take"):
        lax.fori_loop(0, nz, take_step, 0)
    with jax.named_scope("total"):
        total[...] = summed[...].astype(BF16)

    with jax.named_scope("drain"):
        for d in range(1, nr):
            gather_copy(d).wait_send()

        @pl.when(has_next)
        def _():
            tail.wait_send()

        @pl.when(has_prev)
        def _():
            head.wait_send()

        def sent_step(t, carry):
            pair_copy(t).wait_send()

            direct = t != z
            if relayed:
                direct &= ~(hands_up(t) | hands_down(t))

                @pl.when(hands_up(t))
                def _():
                    up_copy().wait_send()

                @pl.when(hands_down(t))
                def _():
                    down_copy().wait_send()

            @pl.when(direct)
            def _():
                far_copy(t).wait_send()

            return carry

        lax.fori_loop(0, nz, sent_step, 0)


def finish(near_sum, wide, total, out, held, sem):
    clusters, leaf, _ = held.shape

    def copy(k):
        return pltpu.make_async_copy(held.at[k], out.at[pl.ds(pl.multiple_of(k * leaf, leaf), leaf)], sem.at[k])

    for k in range(clusters):
        held[k] = (near_sum[k] + dot(wide[k], total[...])).astype(BF16)
        copy(k).start()
    for k in range(clusters):
        copy(k).wait()


def on_device(nr, nc, panel, row_basis, col_basis, near_blocks, couplings, blk_rows, blk_cols, blk_count):
    own_rows, width = panel.shape
    clusters, near_count, leaf, _ = near_blocks.shape
    half = near_count // 2
    rank = col_basis.shape[1]
    slots = couplings.shape[2]
    nz = nc // 2
    block = rank * clusters
    group_rows, group_cols = nc * clusters, nr * clusters
    dma = pltpu.SemaphoreType.DMA
    vmem = pl.BlockSpec(memory_space=pltpu.VMEM)
    near_sum, wide, total = pl.pallas_call(
        functools.partial(kernel, nr, nc),
        out_shape=(
            pltpu.VMEM((clusters, leaf, width), F32),
            pltpu.VMEM((clusters, leaf, block), BF16),
            pltpu.VMEM((block, width), BF16),
        ),
        in_specs=[pl.BlockSpec(memory_space=pl.ANY)] * 7 + [pl.BlockSpec(memory_space=pltpu.HBM)],
        out_specs=[vmem] * 3,
        scratch_shapes=[
            pltpu.VMEM(near_blocks.shape, BF16),
            pltpu.VMEM((clusters + 2 * half, leaf, width), BF16),
            pltpu.VMEM((nc, block, group_cols * rank), BF16),
            pltpu.VMEM((nr, block, width), BF16),
            pltpu.VMEM((clusters, rank, slots), BF16),
            pltpu.VMEM((nr * group_rows, slots), BF16),
            pltpu.VMEM((rank, rank, slots), BF16),
            pltpu.VMEM((rank, own_rows), BF16),
            pltpu.VMEM((rank, own_rows), BF16),
            pltpu.VMEM((1, slots), jnp.int32),
            pltpu.VMEM((1, slots), jnp.int32),
            pltpu.SMEM((1, 1), jnp.int32),
            pltpu.VMEM((nz, block, width), BF16),
            pltpu.VMEM((block, width), F32),
            pltpu.VMEM((nz, block, width), BF16),
            pltpu.VMEM((nz, block, width), BF16),
            pltpu.VMEM((nz, block, width), BF16),
            pltpu.VMEM((block, width), F32),
            pltpu.VMEM((2, block, width), F32),
            pltpu.VMEM((2, block, width), BF16),
            dma((clusters,)),
            dma((8,)),
            dma((max(nr - 1, 1),)),
            dma((max(nr - 1, 1),)),
            dma((2,)),
            dma((2,)),
            dma((nz,)),
            dma((nz,)),
            dma((nz,)),
            dma((nz,)),
            dma((2,)),
            dma((2,)),
            pltpu.SemaphoreType.REGULAR((nr + 1 + nz,)),
        ],
        compiler_params=pltpu.CompilerParams(
            collective_id=0, has_side_effects=True, vmem_limit_bytes=VMEM_BYTES
        ),
    )(
        panel.reshape(clusters, leaf, width),
        row_basis.T,
        col_basis.T,
        near_blocks,
        couplings.reshape(slots, rank, rank).transpose(1, 2, 0),
        blk_rows.reshape(1, slots),
        blk_cols.reshape(1, slots),
        blk_count,
    )
    return pl.pallas_call(
        finish,
        out_shape=jax.ShapeDtypeStruct((own_rows, width), BF16),
        in_specs=[vmem] * 3,
        out_specs=pl.BlockSpec(memory_space=pl.ANY),
        scratch_shapes=[pltpu.VMEM((clusters, leaf, width), BF16), dma((clusters,))],
        compiler_params=pltpu.CompilerParams(vmem_limit_bytes=16 << 20),
    )(near_sum, wide, total)


VMEM_BYTES = 56 << 20


def solution(mesh):
    placed = (
        P(("row", "col"), None),
        P("row", None),
        P(("row", "col"), None),
        P(("row", "col"), None, None, None),
        P("row", "col", None, None, None),
        P("row", "col", None),
        P("row", "col", None),
        P("row", "col"),
    )
    return jax.shard_map(
        functools.partial(on_device, mesh.shape["row"], mesh.shape["col"]),
        mesh=mesh, in_specs=placed, out_specs=P(("row", "col"), None), check_vma=False,
    )
```

```python
import functools

import jax
import jax.numpy as jnp
from jax import lax
from jax.experimental import pallas as pl
from jax.experimental.pallas import tpu as pltpu
from jax.sharding import PartitionSpec as P

MESH = pl.DeviceIdType.MESH
BF16 = jnp.bfloat16
F32 = jnp.float32


def dot(left, right, contract=((1,), (0,))):
    return lax.dot_general(left, right, (contract, ((), ())), preferred_element_type=F32)


def kernel(
    nr, nc,
    panel, row_t, col_t, near, coup, rows, cols, count,
    near_sum, wide, total,
    blocks, win, dense, coeffs, spread, pick,
    coup_v, row_v, col_v, rows_v, cols_v, count_v,
    give, own, pair_in, chip_sum, far_in, summed, kept, relay_in,
    near_sem, in_sem, gs, gr, hs, hr, xs, xr, us, ur, rs, rr, ready,
):
    clusters, near_count, leaf, _ = blocks.shape
    half = near_count // 2
    rank = col_v.shape[0]
    slots = rows_v.shape[1]
    nz = nc // 2
    group_rows = nc * clusters
    group_cols = nr * clusters
    block = rank * clusters
    r = lax.axis_index("row")
    c = lax.axis_index("col")
    line = r * nc + c
    z = c // 2
    e = c % 2
    has_next = line < nr * nc - 1
    has_prev = line > 0
    next_id = (jnp.minimum(line + 1, nr * nc - 1) // nc, (c + 1) % nc)
    prev_id = (jnp.maximum(line - 1, 0) // nc, (c + nc - 1) % nc)
    pair_id = (r, z * 2 + 1 - e)
    lower, upper = e == 0, e == 1
    first, last = z == 0, z == nz - 1
    PAIR, SIDE, LINE = nr - 1, nr, nr + 1
    barrier = pltpu.get_barrier_semaphore()

    def signal(sem, to):
        pl.semaphore_signal(sem, inc=1, device_id=to, device_id_type=MESH)

    def row_id(d):
        return ((r + d) % nr, c)

    with jax.named_scope("greet"):
        for d in range(1, nr):
            @pl.when(r + d < nr)
            def _(d=d):
                signal(barrier, row_id(d))

        @pl.when(lower)
        def _():
            signal(barrier, pair_id)

        for t in range(1, nz):
            @pl.when(t > z)
            def _(t=t):
                signal(barrier, (r, t * 2 + e))

        @pl.when(upper & ~last)
        def _():
            signal(barrier, next_id)

        @pl.when(lower & first & has_prev)
        def _():
            signal(barrier, prev_id)

    own_win = win.at[pl.ds(half, clusters)]
    loads = [
        pltpu.make_async_copy(col_t, col_v, in_sem.at[1]),
        pltpu.make_async_copy(coup, coup_v, in_sem.at[2]),
        pltpu.make_async_copy(rows, rows_v, in_sem.at[3]),
        pltpu.make_async_copy(cols, cols_v, in_sem.at[4]),
        pltpu.make_async_copy(count, count_v, in_sem.at[5]),
        pltpu.make_async_copy(
            row_t.at[:, pl.ds(pl.multiple_of(c * clusters * leaf, 128), clusters * leaf)],
            row_v, in_sem.at[6],
        ),
    ]
    pieces = 2
    per = clusters // pieces
    panel_loads = [
        pltpu.make_async_copy(
            panel.at[pl.ds(p * per, per)], own_win.at[pl.ds(p * per, per)], in_sem.at[(0, 7)[p]]
        )
        for p in range(pieces)
    ]
    with jax.named_scope("loads"):
        loads[0].start()
        for load in panel_loads + loads[1:]:
            load.start()

    def near_load(k):
        return pltpu.make_async_copy(near.at[k], blocks.at[k], near_sem.at[k])

    def start_near(step, carry):
        near_load((step + half) % clusters).start()
        return carry

    tail = pltpu.make_async_remote_copy(
        panel.at[pl.ds(clusters - half, half)], win.at[pl.ds(0, half)], hs.at[0], hr.at[0],
        device_id=next_id, device_id_type=MESH,
    )
    head = pltpu.make_async_remote_copy(
        panel.at[pl.ds(0, half)], win.at[pl.ds(half + clusters, half)], hs.at[1], hr.at[1],
        device_id=prev_id, device_id_type=MESH,
    )

    with jax.named_scope("barrier"):
        one = jnp.int32(1)
        zero = jnp.int32(0)
        earlier = (
            r + z + jnp.where(upper, one, zero)
            + jnp.where(lower & ~first, one, zero) + jnp.where(upper & last & has_next, one, zero)
        )

        @pl.when(earlier > 0)
        def _():
            pl.semaphore_wait(barrier, earlier)

        for d in range(1, nr):
            @pl.when(r + d >= nr)
            def _(d=d):
                signal(ready.at[nr - 1 - d], row_id(d))

        @pl.when(upper)
        def _():
            signal(ready.at[PAIR], pair_id)

        for t in range(nz - 1):
            @pl.when(t < z)
            def _(t=t):
                signal(ready.at[LINE + z], (r, t * 2 + e))

        @pl.when(lower & ~first)
        def _():
            signal(ready.at[SIDE], prev_id)
            head.start()

        @pl.when(upper & last & has_next)
        def _():
            signal(ready.at[SIDE], next_id)

        @pl.when(upper & last & has_next & (r == 0))
        def _():
            tail.start()

        @pl.when(upper)
        def _():
            head.start()

        lax.fori_loop(0, clusters, start_near, 0)

    def gather_copy(d, at=None):
        part = coeffs.at[r] if at is None else coeffs.at[r, pl.ds(at * per * rank, per * rank)]
        return pltpu.make_async_remote_copy(
            part, part, gs.at[d - 1], gr.at[d - 1],
            device_id=row_id(d), device_id_type=MESH,
        )

    with jax.named_scope("panel_wait"):
        loads[0].wait()

    for piece in range(pieces):
        with jax.named_scope("coeffs"):
            panel_loads[piece].wait()
            for k in range(piece * per, (piece + 1) * per):
                coeffs[r, k * rank : (k + 1) * rank, :] = dot(
                    col_v[:, k * leaf : (k + 1) * leaf], win[half + k]
                ).astype(BF16)
        for d in range(1, nr):
            @pl.when(r + d >= nr)
            def _(d=d, piece=piece):
                gather_copy(d, piece).start()

        if piece == 0:
            with jax.named_scope("side"):
                @pl.when(upper & ~last)
                def _():
                    pl.semaphore_wait(ready.at[SIDE], 1)
                    tail.start()

                @pl.when(lower)
                def _():
                    pl.semaphore_wait(ready.at[PAIR], 1)
                    tail.start()

    with jax.named_scope("gather"):
        for d in range(1, nr):
            @pl.when(r + d < nr)
            def _(d=d):
                pl.semaphore_wait(ready.at[d - 1], 1)
                for piece in range(pieces):
                    gather_copy(d, piece).start()

    with jax.named_scope("spread"):
        for load in loads[1:5]:
            load.wait()
        col_ids = cols_v[...]
        live = lax.broadcasted_iota(jnp.int32, (1, slots), 1) < count_v[0, 0]
        picked = jnp.where(live, col_ids // clusters * group_rows + rows_v[...], -1)
        col_ids = col_ids % clusters

        def pick_step(m, carry):
            at = lax.broadcasted_iota(jnp.int32, (clusters, slots), 0) + m * clusters
            hit = jnp.where(at == picked, 1.0, 0.0).astype(BF16)
            pick[pl.ds(pl.multiple_of(m * clusters, clusters), clusters), :] = hit
            return carry

        lax.fori_loop(0, nr * nc, pick_step, 0, unroll=8)
        for j in range(clusters):
            spread[j] = jnp.where(jnp.broadcast_to(col_ids, (rank, slots)) == j, 1.0, 0.0).astype(BF16)

    @pl.when(upper & last & has_next & (r > 0))
    def _():
        tail.start()

    def dense_step(a, carry):
        placed = (spread[...] * coup_v[a][None]).reshape(block, slots)
        part = dot(pick[...], placed, ((1,), (1,))).astype(BF16)
        at = pl.ds(pl.multiple_of(a * clusters, clusters), clusters)
        for s in range(nr):
            dense[:, at, s * block : (s + 1) * block] = part[s * group_rows : (s + 1) * group_rows].reshape(
                nc, clusters, block
            )
        return carry

    with jax.named_scope("dense0"):
        lax.fori_loop(0, rank // 2, dense_step, 0, unroll=2)

    with jax.named_scope("dense1"):
        lax.fori_loop(rank // 2, rank, dense_step, 0, unroll=2)

    def near_step(k, carry):
        near_load(k).wait()
        left = jnp.concatenate([blocks[k, o] for o in range(near_count)], axis=1)
        right = win[pl.ds(k, near_count)].reshape(near_count * leaf, win.shape[2])
        near_sum[k] = dot(left, right)
        return carry

    def wide_step(k, carry):
        at = lax.broadcasted_iota(jnp.int32, (rank, block), 0)
        to = lax.broadcasted_iota(jnp.int32, (rank, block), 1)
        place = jnp.where(to == at * clusters + k, 1.0, 0.0).astype(BF16)
        mine = row_v[:, pl.ds(pl.multiple_of(k * leaf, leaf), leaf)]
        wide[k] = dot(mine, place, ((0,), (0,))).astype(BF16)
        return carry

    with jax.named_scope("wrap"):
        @pl.when(lower & first & has_prev)
        def _():
            pl.semaphore_wait(ready.at[SIDE], 1)
            head.start()

    with jax.named_scope("wide"):
        loads[5].wait()
        lax.fori_loop(0, clusters, wide_step, 0, unroll=4)
    early = half + (clusters - 2 * half) // 4
    with jax.named_scope("near_early"):
        lax.fori_loop(half, early, near_step, 0)

    with jax.named_scope("gather_wait"):
        for d in range(1, nr):
            gather_copy(d).wait_recv()

    relayed = nz > 2
    up_to, down_to = 2, nz - 3

    def target(j):
        far_first = jnp.where(z < nz // 2, nz - 1 - j, j)
        if not relayed:
            return far_first
        skip = nz - j
        apart = jnp.where(j == 0, up_to, jnp.where(skip > up_to, skip, skip - 1))
        near_first = jnp.where(j == 0, 0, nz - j)
        inner = jnp.where(z < nz // 2, near_first, far_first)
        return jnp.where(first, apart, jnp.where(last, nz - 1 - apart, inner))

    def hands_up(t):
        return first & (t == up_to) if relayed else False

    def hands_down(t):
        return last & (t == down_to) if relayed else False

    def partial_for(column):
        return dot(dense[column], coeffs[...].reshape(group_cols * rank, coeffs.shape[2]))

    def pair_copy(t):
        return pltpu.make_async_remote_copy(
            give.at[t], pair_in.at[t], xs.at[t], xr.at[t], device_id=pair_id, device_id_type=MESH
        )

    def far_copy(t):
        return pltpu.make_async_remote_copy(
            chip_sum.at[t], far_in.at[z], us.at[t], ur.at[z],
            device_id=(r, t * 2 + e), device_id_type=MESH,
        )

    def give_step(j, carry):
        t = target(j)
        give[t] = partial_for(t * 2 + 1 - e).astype(BF16)
        pair_copy(t).start()
        return carry

    with jax.named_scope("give"):
        for t in range(1, nz):
            @pl.when(t > z)
            def _(t=t):
                pl.semaphore_wait(ready.at[LINE + t], 1)

        lax.fori_loop(0, nz, give_step, 0)

    def up_copy():
        return pltpu.make_async_remote_copy(
            chip_sum.at[up_to], relay_in.at[0], rs.at[0], rr.at[0],
            device_id=(r, 2 + e), device_id_type=MESH,
        )

    def down_copy():
        return pltpu.make_async_remote_copy(
            chip_sum.at[down_to], relay_in.at[1], rs.at[1], rr.at[1],
            device_id=(r, (nz - 2) * 2 + e), device_id_type=MESH,
        )

    def send_step(j, carry):
        t = target(j)
        own[...] = partial_for(t * 2 + e)
        pair_copy(t).wait_recv()
        value = own[...] + pair_in[t].astype(F32)
        direct = t != z
        if relayed:
            keeps_up = (z == 1) & (t == up_to)
            keeps_down = (z == nz - 2) & (t == down_to)
            direct &= ~(keeps_up | keeps_down)

            @pl.when(keeps_up)
            def _():
                kept[0] = value

            @pl.when(keeps_down)
            def _():
                kept[1] = value

        @pl.when(t == z)
        def _():
            summed[...] = value

        @pl.when(direct)
        def _():
            chip_sum[t] = value.astype(BF16)

            if relayed:
                @pl.when(hands_up(t))
                def _():
                    up_copy().start()

                @pl.when(hands_down(t))
                def _():
                    down_copy().start()

                @pl.when(~(hands_up(t) | hands_down(t)))
                def _():
                    far_copy(t).start()
            else:
                far_copy(t).start()

        return carry

    with jax.named_scope("send"):
        lax.fori_loop(0, nz, send_step, 0)

    with jax.named_scope("near0"):
        lax.fori_loop(early, clusters - half, near_step, 0)

    def relay():
        @pl.when(z == 1)
        def _():
            up_copy().wait_recv()
            chip_sum[up_to] = (kept[0] + relay_in[0].astype(F32)).astype(BF16)
            far_copy(up_to).start()

        @pl.when(z == nz - 2)
        def _():
            down_copy().wait_recv()
            chip_sum[down_to] = (kept[1] + relay_in[1].astype(F32)).astype(BF16)
            far_copy(down_to).start()

    def take_front():
        @pl.when(has_prev)
        def _():
            tail.wait_recv()

        @pl.when(~has_prev)
        def _():
            win[pl.ds(0, half)] = jnp.zeros((half, leaf, win.shape[2]), BF16)

    def take_back():
        @pl.when(has_next)
        def _():
            head.wait_recv()

        @pl.when(~has_next)
        def _():
            win[pl.ds(half + clusters, half)] = jnp.zeros((half, leaf, win.shape[2]), BF16)

    def edge_step(base):
        def step(k, carry):
            return near_step(base + k, carry)
        return step

    with jax.named_scope("near1"):
        pl.when(lower)(take_back)
        pl.when(upper)(take_front)
        lax.fori_loop(0, half, edge_step(jnp.where(lower, clusters - half, 0)), 0)
    if relayed:
        with jax.named_scope("relay"):
            relay()
    with jax.named_scope("halo_wait"):
        pl.when(upper)(take_back)
        pl.when(lower)(take_front)
    with jax.named_scope("near2"):
        lax.fori_loop(0, half, edge_step(jnp.where(lower, 0, clusters - half)), 0)

    def take_step(j, carry):
        s = jnp.where(z < nz // 2, j, nz - 1 - j)
        direct = s != z
        if relayed:
            direct &= ~(((z == up_to) & (s == 0)) | ((z == down_to) & (s == nz - 1)))

        @pl.when(direct)
        def _():
            pltpu.make_async_remote_copy(
                chip_sum.at[s], far_in.at[s], us.at[s], ur.at[s],
                device_id=(r, s * 2 + e), device_id_type=MESH,
            ).wait_recv()
            summed[...] += far_in[s].astype(F32)

        return carry

    with jax.named_scope("take"):
        lax.fori_loop(0, nz, take_step, 0)
    with jax.named_scope("total"):
        total[...] = summed[...].astype(BF16)

    with jax.named_scope("drain"):
        for d in range(1, nr):
            gather_copy(d).wait_send()

        @pl.when(has_next)
        def _():
            tail.wait_send()

        @pl.when(has_prev)
        def _():
            head.wait_send()

        def sent_step(t, carry):
            pair_copy(t).wait_send()

            direct = t != z
            if relayed:
                direct &= ~(hands_up(t) | hands_down(t))

                @pl.when(hands_up(t))
                def _():
                    up_copy().wait_send()

                @pl.when(hands_down(t))
                def _():
                    down_copy().wait_send()

            @pl.when(direct)
            def _():
                far_copy(t).wait_send()

            return carry

        lax.fori_loop(0, nz, sent_step, 0)


def finish(near_sum, wide, total, out, held, sem):
    clusters, leaf, _ = held.shape

    def copy(k):
        return pltpu.make_async_copy(held.at[k], out.at[pl.ds(pl.multiple_of(k * leaf, leaf), leaf)], sem.at[k])

    for k in range(clusters):
        held[k] = (near_sum[k] + dot(wide[k], total[...])).astype(BF16)
        copy(k).start()
    for k in range(clusters):
        copy(k).wait()


def on_device(nr, nc, panel, row_basis, col_basis, near_blocks, couplings, blk_rows, blk_cols, blk_count):
    own_rows, width = panel.shape
    clusters, near_count, leaf, _ = near_blocks.shape
    half = near_count // 2
    rank = col_basis.shape[1]
    slots = couplings.shape[2]
    nz = nc // 2
    block = rank * clusters
    group_rows, group_cols = nc * clusters, nr * clusters
    dma = pltpu.SemaphoreType.DMA
    vmem = pl.BlockSpec(memory_space=pltpu.VMEM)
    near_sum, wide, total = pl.pallas_call(
        functools.partial(kernel, nr, nc),
        out_shape=(
            pltpu.VMEM((clusters, leaf, width), F32),
            pltpu.VMEM((clusters, leaf, block), BF16),
            pltpu.VMEM((block, width), BF16),
        ),
        in_specs=[pl.BlockSpec(memory_space=pl.ANY)] * 7 + [pl.BlockSpec(memory_space=pltpu.HBM)],
        out_specs=[vmem] * 3,
        scratch_shapes=[
            pltpu.VMEM(near_blocks.shape, BF16),
            pltpu.VMEM((clusters + 2 * half, leaf, width), BF16),
            pltpu.VMEM((nc, block, group_cols * rank), BF16),
            pltpu.VMEM((nr, block, width), BF16),
            pltpu.VMEM((clusters, rank, slots), BF16),
            pltpu.VMEM((nr * group_rows, slots), BF16),
            pltpu.VMEM((rank, rank, slots), BF16),
            pltpu.VMEM((rank, own_rows), BF16),
            pltpu.VMEM((rank, own_rows), BF16),
            pltpu.VMEM((1, slots), jnp.int32),
            pltpu.VMEM((1, slots), jnp.int32),
            pltpu.SMEM((1, 1), jnp.int32),
            pltpu.VMEM((nz, block, width), BF16),
            pltpu.VMEM((block, width), F32),
            pltpu.VMEM((nz, block, width), BF16),
            pltpu.VMEM((nz, block, width), BF16),
            pltpu.VMEM((nz, block, width), BF16),
            pltpu.VMEM((block, width), F32),
            pltpu.VMEM((2, block, width), F32),
            pltpu.VMEM((2, block, width), BF16),
            dma((clusters,)),
            dma((8,)),
            dma((max(nr - 1, 1),)),
            dma((max(nr - 1, 1),)),
            dma((2,)),
            dma((2,)),
            dma((nz,)),
            dma((nz,)),
            dma((nz,)),
            dma((nz,)),
            dma((2,)),
            dma((2,)),
            pltpu.SemaphoreType.REGULAR((nr + 1 + nz,)),
        ],
        compiler_params=pltpu.CompilerParams(
            collective_id=0, has_side_effects=True, vmem_limit_bytes=VMEM_BYTES
        ),
    )(
        panel.reshape(clusters, leaf, width),
        row_basis.T,
        col_basis.T,
        near_blocks,
        couplings.reshape(slots, rank, rank).transpose(1, 2, 0),
        blk_rows.reshape(1, slots),
        blk_cols.reshape(1, slots),
        blk_count,
    )
    return pl.pallas_call(
        finish,
        out_shape=jax.ShapeDtypeStruct((own_rows, width), BF16),
        in_specs=[vmem] * 3,
        out_specs=pl.BlockSpec(memory_space=pl.ANY),
        scratch_shapes=[pltpu.VMEM((clusters, leaf, width), BF16), dma((clusters,))],
        compiler_params=pltpu.CompilerParams(vmem_limit_bytes=16 << 20),
    )(near_sum, wide, total)


VMEM_BYTES = 56 << 20


def solution(mesh):
    placed = (
        P(("row", "col"), None),
        P("row", None),
        P(("row", "col"), None),
        P(("row", "col"), None, None, None),
        P("row", "col", None, None, None),
        P("row", "col", None),
        P("row", "col", None),
        P("row", "col"),
    )
    return jax.shard_map(
        functools.partial(on_device, mesh.shape["row"], mesh.shape["col"]),
        mesh=mesh, in_specs=placed, out_specs=P(("row", "col"), None), check_vma=False,
    )
```
